32 devices in a mesh: mem: 8 (over z, x), chan: 4 (over y, core).
Axes of the slice: x: 2, y: 2, z: 4, core: 2. Of those that a mesh axis runs over, the one named last changes fastest.
Arguments:
- state_anom: bfloat16 [8, 64, 137], P(None, 'mem'), may hold values from -6 to 6
- radiance_anom: bfloat16 [8, 64, 8704], P(None, 'mem', 'chan'), may hold values from -6 to 6
- inv_noise: float32 [8704], P('chan'), may hold values from 0.02 to 0.2
- innovation: float32 [8, 8704], P(None, 'chan'), may hold values from -6 to 6
- valid_count: int32 [8], replicated, may hold values from 4352 to 8461
Outputs:
- information: float32 [8, 137, 137], P('mem')
- gradient: float32 [8, 137], P('mem')
- increment: float32 [8, 137], P('mem')
The draws below stay inside these ranges and needn't reach their ends.
All inputs are finite; a program needn't handle non-finite values.
Results may differ from the reference program's by a relative error of at most 0.0003.
Values may be sent and summed in bfloat16 or wider, within the bound.
A program may use at most 64 MiB of HBM per device.

```python
import math
import jax
import jax.numpy as jnp
from jax import lax

STATE = 137
PROF = 8
MEMBERS = 64
CHANNELS = 8704


def place_ends(result, own_key, low, top_value):
    place = [jax.random.randint(jax.random.fold_in(own_key, axis), (), 0, length) for axis, length in enumerate(result.shape)]
    longest = result.shape.index(max(result.shape))
    neighbour = place[:longest] + [(place[longest] + 1) % result.shape[longest]] + place[longest + 1:]
    return result.at[tuple(place)].set(low).at[tuple(neighbour)].set(top_value)


def levels(stream_key, dims, pieces, least, top_value):
    loudness, own = 1.0, jax.random.fold_in(stream_key, 6)
    for position, shards_of in pieces:
        heights = jnp.exp(jax.random.uniform(jax.random.fold_in(own, position), (shards_of,), jnp.float32, least / len(pieces), top_value / len(pieces)))
        loudness = loudness * jnp.repeat(heights, dims[position] // shards_of).reshape([-1 if axis == position else 1 for axis in range(len(dims))])
    return loudness


def bell_draw(rng, dims, deviation, reach, pieces=(), held_as=jnp.bfloat16):
    array = jax.random.normal(rng, dims, jnp.float32) * deviation
    if len(pieces) > 0:
        array = levels(rng, dims, pieces, -0.22, 0.18) * array
    return jnp.clip(array, min=-reach, max=reach).astype(held_as)


def setup_inputs(seed: int = 0) -> dict:
    keys = jax.random.split(jax.random.key(seed), 6)
    return {
        "state_anom": bell_draw(keys[0], (PROF, MEMBERS, STATE), 1.0, 6.0, ((1, 8),)),
        "radiance_anom": bell_draw(keys[1], (PROF, MEMBERS, CHANNELS), 1.0, 6.0, ((1, 8), (2, 4))),
        "inv_noise": jnp.clip(jnp.exp(math.log(0.2) - 2.3025851 * jax.random.uniform(keys[2], (CHANNELS,), jnp.float32) ** levels(keys[2], (CHANNELS,), ((0, 4),), -0.2, 0.2)), 0.02, 0.2),
        "innovation": bell_draw(keys[3], (PROF, CHANNELS), 1.0, 6.0, ((1, 4),), jnp.float32),
        "valid_count": place_ends(jax.random.randint(keys[4], (PROF,), CHANNELS // 2, min(CHANNELS, 8461) + 1), jax.random.fold_in(keys[4], 1), CHANNELS // 2, min(CHANNELS, 8461)).astype(jnp.int32),
    }


def reference(state_anom, radiance_anom, inv_noise, innovation, valid_count):
    cross = jnp.einsum('pmc,pms->pcs', radiance_anom.astype(jnp.float32), state_anom.astype(jnp.float32), precision=lax.Precision.HIGHEST)
    cross = cross / jnp.float32(MEMBERS - 1)
    slots = jnp.arange(CHANNELS, dtype=jnp.int32)
    valid = (slots[None, :] < valid_count[:, None].astype(jnp.int32)).astype(jnp.float32)
    weight = inv_noise[None, :] * valid
    weighted = cross * weight[:, :, None]
    information = jnp.einsum('pcs,pct->pst', weighted, cross, precision=lax.Precision.HIGHEST)
    gradient = jnp.einsum('pcs,pc->ps', weighted, innovation, precision=lax.Precision.HIGHEST)
    system = information + jnp.eye(STATE, dtype=jnp.float32)[None]
    increment = jnp.linalg.solve(system, gradient[:, :, None])[:, :, 0]
    return (information, gradient, increment)
```

```python
import functools
import jax
import jax.numpy as jnp
from jax import lax
from jax.experimental import pallas as pl
from jax.experimental.pallas import tpu as pltpu
from jax.sharding import PartitionSpec as P

F32, BF16 = jnp.float32, jnp.bfloat16
LANES, SUB = 128, 8
VMEM_LIMIT = 60 * 1024 * 1024


def up(x, to):
    return -(-x // to) * to


def split3(x):
    a = x.astype(BF16)
    rest = x - a.astype(F32)
    b = rest.astype(BF16)
    c = (rest - b.astype(F32)).astype(BF16)
    return a, b, c


def gram_kernel(n_mem, n_chan, count_ref, state_ref, rad_ref, noise_ref, innov_ref,
                gram_ref, states_ref, held, held_states, innov, parts,
                local_sem, send_sem, recv_sem, ssend_sem, srecv_sem, psend_sem, precv_sem):
    me, slab = lax.axis_index("mem"), lax.axis_index("chan")
    members = rad_ref.shape[1]
    width = rad_ref.shape[2]
    total = n_mem * members
    columns = parts.shape[2]

    barrier = pltpu.get_barrier_semaphore()
    for k in range(1, n_mem):
        pl.semaphore_signal(barrier, inc=1, device_id={"mem": lax.rem(me + k, n_mem)})
    for k in range(1, n_chan):
        pl.semaphore_signal(barrier, inc=1, device_id={"chan": lax.rem(slab + k, n_chan)})
    own = [
        pltpu.make_async_copy(rad_ref.at[me], held.at[0], local_sem.at[0]),
        pltpu.make_async_copy(state_ref.at[me], held_states.at[0], local_sem.at[1]),
        pltpu.make_async_copy(innov_ref, innov, local_sem.at[2]),
    ]
    for copy in own:
        copy.start()
    pl.semaphore_wait(barrier, n_mem - 1 + n_chan - 1)

    sends = []
    for k in range(1, n_mem):
        peer = lax.rem(me + k, n_mem)
        sends.append(pltpu.make_async_remote_copy(
            src_ref=rad_ref.at[peer], dst_ref=held.at[k],
            send_sem=send_sem.at[k], recv_sem=recv_sem.at[k], device_id={"mem": peer}))
        sends[-1].start()
    for k in range(1, n_mem):
        peer = lax.rem(me + k, n_mem)
        sends.append(pltpu.make_async_remote_copy(
            src_ref=state_ref.at[peer], dst_ref=held_states.at[k],
            send_sem=ssend_sem.at[k], recv_sem=srecv_sem.at[k], device_id={"mem": peer}))
        sends[-1].start()

    for copy in own:
        copy.wait()
    slots = slab * width + lax.broadcasted_iota(jnp.int32, (1, width), 1)
    weight = jnp.where(slots < count_ref[me], noise_ref[...], 0.0)
    pull = weight * innov[pl.ds(me, 1), :]
    pull = [part.astype(F32) for part in split3(pull)]
    for copy in sends:
        copy.wait_recv()

    extra = columns - total
    row = lax.broadcasted_iota(jnp.int32, (extra, 1), 0)
    acc = jnp.zeros((total, columns), F32)
    step = 2 * LANES
    for lo in range(0, width, step):
        hi = min(lo + step, width)
        block = held[:, :, lo:hi].astype(F32).reshape(total, hi - lo)
        scaled = block * weight[:, lo:hi]
        first = scaled.astype(BF16)
        second = (scaled - first.astype(F32)).astype(BF16)
        p0, p1, p2 = (part[:, lo:hi] for part in pull)
        tail0 = jnp.where(row == 0, p0, jnp.where(row == 1, p2, 0.0)).astype(BF16)
        tail1 = jnp.where(row == 0, p1, 0.0).astype(BF16)
        block = block.astype(BF16)
        dims = (((1,), (1,)), ((), ()))
        acc += (
            lax.dot_general(block, jnp.concatenate([first, tail0], 0), dims, preferred_element_type=F32)
            + lax.dot_general(block, jnp.concatenate([second, tail1], 0), dims, preferred_element_type=F32)
        )
    parts[slab] = acc
    states_ref[...] = held_states[...]

    shares = []
    for k in range(1, n_chan):
        peer = lax.rem(slab + k, n_chan)
        shares.append(pltpu.make_async_remote_copy(
            src_ref=parts.at[slab], dst_ref=parts.at[slab],
            send_sem=psend_sem.at[k], recv_sem=precv_sem.at[k], device_id={"chan": peer}))
        shares[-1].start()
    for copy in sends:
        copy.wait_send()
    for copy in shares:
        copy.wait()
    whole = parts[0]
    for k in range(1, n_chan):
        whole = whole + parts[k]
    gram_ref[...] = whole


def eliminate(system, order):
    rows, lanes = system.shape
    rid = lax.broadcasted_iota(jnp.int32, (SUB, LANES), 0)

    def wide(piece, tiles):
        return piece if tiles == 1 else jnp.concatenate([piece] * tiles, 1)

    for p in range(0, order, SUB):
        steps = min(SUB, order - p)
        base = p // LANES * LANES
        live = system[:, base:]
        tiles = (lanes - base) // LANES
        cols = []
        for j in range(steps):
            at = p - base + j
            full = jnp.broadcast_to(live[:, at:at + 1], (rows, LANES))
            cols.append([full[:p], full[p:p + SUB], full[p + SUB:]])
        block = live[p:p + SUB]
        above, below = live[:p], live[p + SUB:]
        for j in range(steps):
            inverse = 1.0 / cols[j][1][j:j + 1, :]
            pivot_row = block[j:j + 1, :] * wide(inverse, tiles)
            for later in range(j + 1, steps):
                c = cols[later]
                scale = c[1][j:j + 1, :] * inverse
                cols[later] = [
                    c[0] - cols[j][0] * scale if p else c[0],
                    jnp.where(rid == j, jnp.broadcast_to(scale, (SUB, LANES)), c[1] - cols[j][1] * scale),
                    c[2] - cols[j][2] * scale if p + SUB < rows else c[2],
                ]
            block = jnp.where(wide(rid, tiles) == j, jnp.broadcast_to(pivot_row, block.shape),
                              block - wide(cols[j][1], tiles) * pivot_row)
            if p:
                above = above - wide(cols[j][0], tiles) * pivot_row
            if p + SUB < rows:
                below = below - wide(cols[j][2], tiles) * pivot_row
        pieces = ([above] if p else []) + [block] + ([below] if p + SUB < rows else [])
        live = jnp.concatenate(pieces, 0) if len(pieces) > 1 else pieces[0]
        system = live if base == 0 else jnp.concatenate([system[:, :base], live], 1)
    return system[:, order:order + 1]


def solve_kernel(total, gram_ref, states_ref, info_ref, grad_ref, inc_ref):
    states = states_ref.shape[2]
    columns = gram_ref.shape[1]
    scale = 1.0 / (total - 1)
    rows, lanes = up(states, SUB), up(states + 1, LANES)
    anom = states_ref[...].astype(F32).reshape(total, states)
    anom = jnp.concatenate([anom, jnp.zeros((total, lanes - states), F32)], 1)
    turned = anom.T[:rows].astype(BF16)
    anom = jnp.concatenate([anom, jnp.zeros((columns - total, lanes), F32)], 0).astype(BF16)
    half = functools.reduce(
        lambda a, b: b + a,
        [jnp.dot(turned, g, preferred_element_type=F32) for g in split3(gram_ref[...])][::-1])
    grad = (half[:, total:total + 1] + half[:, total + 1:total + 2]) * scale
    info = functools.reduce(
        lambda a, b: b + a,
        [jnp.dot(h, anom, preferred_element_type=F32) for h in split3(half)][::-1])
    info = info * (scale * scale)
    info_ref[0] = info[:states, :states]
    rid = lax.broadcasted_iota(jnp.int32, (rows, lanes), 0)
    cid = lax.broadcasted_iota(jnp.int32, (rows, lanes), 1)
    system = info + jnp.where(rid == cid, 1.0, 0.0)
    system = jnp.where(cid == states, jnp.broadcast_to(grad, (rows, lanes)), system)
    step = eliminate(system, states)
    lid = lax.broadcasted_iota(jnp.int32, (rows, LANES), 1)
    pair = jnp.where(lid == 0, grad, jnp.where(lid == 1, step, 0.0))
    pair = jnp.concatenate([pair, jnp.zeros((lanes - rows, LANES), F32)], 0).T
    grad_ref[...] = pair[0:1, :states]
    inc_ref[...] = pair[1:2, :states]


def shards(state_anom, radiance_anom, inv_noise, innovation, valid_count):
    n_mem, n_chan = lax.axis_size("mem"), lax.axis_size("chan")
    members, states = state_anom.shape[1:]
    width = radiance_anom.shape[2]
    total = members * n_mem
    columns = up(total + 16, LANES)
    vmem, anywhere = pl.BlockSpec(memory_space=pltpu.VMEM), pl.BlockSpec(memory_space=pl.ANY)
    dma = pltpu.SemaphoreType.DMA
    gram, own_states = pl.pallas_call(
        functools.partial(gram_kernel, n_mem, n_chan),
        out_shape=(jax.ShapeDtypeStruct((total, columns), F32),
                   jax.ShapeDtypeStruct((n_mem, members, states), BF16)),
        in_specs=[pl.BlockSpec(memory_space=pltpu.SMEM), anywhere, anywhere, vmem, anywhere],
        out_specs=(vmem, vmem),
        scratch_shapes=[
            pltpu.VMEM((n_mem, members, width), BF16),
            pltpu.VMEM((n_mem, members, states), BF16),
            pltpu.VMEM(innovation.shape, F32),
            pltpu.VMEM((n_chan, total, columns), F32),
            dma((3,)), dma((n_mem,)), dma((n_mem,)), dma((n_mem,)), dma((n_mem,)),
            dma((n_chan,)), dma((n_chan,)),
        ],
        compiler_params=pltpu.CompilerParams(
            collective_id=0, has_side_effects=True, vmem_limit_bytes=VMEM_LIMIT),
    )(valid_count, state_anom, radiance_anom, inv_noise[None, :], innovation)
    return pl.pallas_call(
        functools.partial(solve_kernel, total),
        out_shape=(jax.ShapeDtypeStruct((1, states, states), F32),
                   jax.ShapeDtypeStruct((1, states), F32),
                   jax.ShapeDtypeStruct((1, states), F32)),
        in_specs=[vmem, vmem],
        out_specs=(vmem, vmem, vmem),
        compiler_params=pltpu.CompilerParams(vmem_limit_bytes=VMEM_LIMIT),
    )(gram, own_states)


def solution(mesh):
    in_specs = (P(None, "mem", None), P(None, "mem", "chan"), P("chan"), P(None, "chan"), P())
    out_specs = (P("mem", None, None), P("mem", None), P("mem", None))
    return jax.shard_map(shards, mesh=mesh, in_specs=in_specs, out_specs=out_specs, check_vma=False)
```

```python
import functools
import jax
import jax.numpy as jnp
from jax import lax
from jax.experimental import pallas as pl
from jax.experimental.pallas import tpu as pltpu
from jax.sharding import PartitionSpec as P

F32, BF16 = jnp.float32, jnp.bfloat16
LANES, SUB = 128, 8
PARTS = 4
VMEM_LIMIT = 60 * 1024 * 1024


def up(x, to):
    return -(-x // to) * to


def split3(x):
    a = x.astype(BF16)
    rest = x - a.astype(F32)
    b = rest.astype(BF16)
    c = (rest - b.astype(F32)).astype(BF16)
    return a, b, c


def pieces(width, count):
    tiles = width // LANES
    marks = [(tiles - tiles * i // count) * LANES for i in range(count, 0, -1)] + [width]
    return list(zip(marks[:-1], marks[1:]))


def gram_kernel(n_mem, n_chan, parts_of_slab, count_ref, state_ref, rad_ref, noise_ref, innov_ref,
                gram_ref, states_ref, held, held_states, innov, parts,
                local_sem, send_sem, recv_sem, ssend_sem, srecv_sem, psend_sem, precv_sem):
    me, slab = lax.axis_index("mem"), lax.axis_index("chan")
    members = rad_ref.shape[1]
    width = rad_ref.shape[2]
    total = n_mem * members
    columns = parts.shape[2]

    barrier = pltpu.get_barrier_semaphore()
    for k in range(1, n_mem):
        pl.semaphore_signal(barrier, inc=1, device_id={"mem": lax.rem(me + k, n_mem)})
    for k in range(1, n_chan):
        pl.semaphore_signal(barrier, inc=1, device_id={"chan": lax.rem(slab + k, n_chan)})
    own = [
        pltpu.make_async_copy(rad_ref.at[me], held.at[0], local_sem.at[0]),
        pltpu.make_async_copy(state_ref.at[me], held_states.at[0], local_sem.at[1]),
        pltpu.make_async_copy(innov_ref, innov, local_sem.at[2]),
    ]
    for copy in own:
        copy.start()
    pl.semaphore_wait(barrier, n_mem - 1 + n_chan - 1)

    cuts = pieces(width, parts_of_slab)
    sends, late = [], []
    for c, (lo, hi) in enumerate(cuts):
        for k in range(n_mem - 1, 0, -1):
            peer = lax.rem(me + k, n_mem)
            late.append(pltpu.make_async_remote_copy(
                src_ref=rad_ref.at[peer, :, lo:hi], dst_ref=held.at[k, :, lo:hi],
                send_sem=send_sem.at[c, k], recv_sem=recv_sem.at[c, k], device_id={"mem": peer}))
            late[-1].start()
        sends.append(late)
        late = []
    small = []
    for k in range(1, n_mem):
        peer = lax.rem(me + k, n_mem)
        small.append(pltpu.make_async_remote_copy(
            src_ref=state_ref.at[peer], dst_ref=held_states.at[k],
            send_sem=ssend_sem.at[k], recv_sem=srecv_sem.at[k], device_id={"mem": peer}))
        small[-1].start()

    for copy in own:
        copy.wait()
    slots = slab * width + lax.broadcasted_iota(jnp.int32, (1, width), 1)
    weight = jnp.where(slots < count_ref[me], noise_ref[...].reshape(1, width), 0.0)
    pull = weight * innov[pl.ds(me, 1), :]
    pull = [part.astype(F32) for part in split3(pull)]
    extra = columns - total
    row = lax.broadcasted_iota(jnp.int32, (extra, 1), 0)
    acc = jnp.zeros((total, columns), F32)
    step = 2 * LANES
    for (start, stop), copies in zip(cuts, sends):
        for copy in copies:
            copy.wait_recv()
        for lo in range(start, stop, step):
            hi = min(lo + step, stop)
            block = held[:, :, lo:hi].astype(F32).reshape(total, hi - lo)
            scaled = block * weight[:, lo:hi]
            first = scaled.astype(BF16)
            second = (scaled - first.astype(F32)).astype(BF16)
            p0, p1, p2 = (part[:, lo:hi] for part in pull)
            tail0 = jnp.where(row == 0, p0, jnp.where(row == 1, p2, 0.0)).astype(BF16)
            tail1 = jnp.where(row == 0, p1, 0.0).astype(BF16)
            block = block.astype(BF16)
            dims = (((1,), (1,)), ((), ()))
            acc += (
                lax.dot_general(block, jnp.concatenate([first, tail0], 0), dims, preferred_element_type=F32)
                + lax.dot_general(block, jnp.concatenate([second, tail1], 0), dims, preferred_element_type=F32)
            )
    parts[slab] = acc

    shares = []
    for k in range(1, n_chan):
        peer = lax.rem(slab + k, n_chan)
        shares.append(pltpu.make_async_remote_copy(
            src_ref=parts.at[slab], dst_ref=parts.at[slab],
            send_sem=psend_sem.at[k], recv_sem=precv_sem.at[k], device_id={"chan": peer}))
        shares[-1].start()
    for copy in small:
        copy.wait_recv()
    states_ref[...] = held_states[...]
    for copy in small + sum(sends, []):
        copy.wait_send()
    for copy in shares:
        copy.wait()
    whole = parts[0]
    for k in range(1, n_chan):
        whole = whole + parts[k]
    gram_ref[...] = whole


def eliminate(system, order):
    rows, lanes = system.shape
    rid = lax.broadcasted_iota(jnp.int32, (SUB, LANES), 0)

    def wide(piece, tiles):
        return piece if tiles == 1 else jnp.concatenate([piece] * tiles, 1)

    for p in range(0, order, SUB):
        steps = min(SUB, order - p)
        base = p // LANES * LANES
        live = system[:, base:]
        tiles = (lanes - base) // LANES
        cols = []
        for j in range(steps):
            at = p - base + j
            full = jnp.broadcast_to(live[:, at:at + 1], (rows, LANES))
            cols.append([full[:p], full[p:p + SUB], full[p + SUB:]])
        block = live[p:p + SUB]
        above, below = live[:p], live[p + SUB:]
        for j in range(steps):
            inverse = 1.0 / cols[j][1][j:j + 1, :]
            pivot_row = block[j:j + 1, :] * wide(inverse, tiles)
            for later in range(j + 1, steps):
                c = cols[later]
                scale = c[1][j:j + 1, :] * inverse
                cols[later] = [
                    c[0] - cols[j][0] * scale if p else c[0],
                    jnp.where(rid == j, jnp.broadcast_to(scale, (SUB, LANES)), c[1] - cols[j][1] * scale),
                    c[2] - cols[j][2] * scale if p + SUB < rows else c[2],
                ]
            block = jnp.where(wide(rid, tiles) == j, jnp.broadcast_to(pivot_row, block.shape),
                              block - wide(cols[j][1], tiles) * pivot_row)
            if p:
                above = above - wide(cols[j][0], tiles) * pivot_row
            if p + SUB < rows:
                below = below - wide(cols[j][2], tiles) * pivot_row
        pieces = ([above] if p else []) + [block] + ([below] if p + SUB < rows else [])
        live = jnp.concatenate(pieces, 0) if len(pieces) > 1 else pieces[0]
        system = live if base == 0 else jnp.concatenate([system[:, :base], live], 1)
    return system[:, order:order + 1]


def solve_kernel(total, gram_ref, states_ref, info_ref, grad_ref, inc_ref):
    states = states_ref.shape[2]
    columns = gram_ref.shape[1]
    scale = 1.0 / (total - 1)
    rows, lanes = up(states, SUB), up(states + 1, LANES)
    anom = states_ref[...].astype(F32).reshape(total, states)
    anom = jnp.concatenate([anom, jnp.zeros((total, lanes - states), F32)], 1)
    turned = anom.T[:rows].astype(BF16)
    anom = jnp.concatenate([anom, jnp.zeros((columns - total, lanes), F32)], 0).astype(BF16)
    half = functools.reduce(
        lambda a, b: b + a,
        [jnp.dot(turned, g, preferred_element_type=F32) for g in split3(gram_ref[...])][::-1])
    grad = (half[:, total:total + 1] + half[:, total + 1:total + 2]) * scale
    info = functools.reduce(
        lambda a, b: b + a,
        [jnp.dot(h, anom, preferred_element_type=F32) for h in split3(half)][::-1])
    info = info * (scale * scale)
    info_ref[:, 0, :] = info[:states, :states]
    rid = lax.broadcasted_iota(jnp.int32, (rows, lanes), 0)
    cid = lax.broadcasted_iota(jnp.int32, (rows, lanes), 1)
    system = info + jnp.where(rid == cid, 1.0, 0.0)
    system = jnp.where(cid == states, jnp.broadcast_to(grad, (rows, lanes)), system)
    step = eliminate(system, states)
    lid = lax.broadcasted_iota(jnp.int32, (rows, LANES), 1)
    pair = jnp.where(lid == 0, grad, jnp.where(lid == 1, step, 0.0))
    pair = jnp.concatenate([pair, jnp.zeros((lanes - rows, LANES), F32)], 0).T
    grad_ref[...] = pair[0:1, :states]
    inc_ref[...] = pair[1:2, :states]


def shards(state_anom, radiance_anom, inv_noise, innovation, valid_count):
    n_mem, n_chan = lax.axis_size("mem"), lax.axis_size("chan")
    members, states = state_anom.shape[1:]
    width = radiance_anom.shape[2]
    total = members * n_mem
    columns = up(total + 16, LANES)
    vmem, anywhere = pl.BlockSpec(memory_space=pltpu.VMEM), pl.BlockSpec(memory_space=pl.ANY)
    dma = pltpu.SemaphoreType.DMA
    gram, own_states = pl.pallas_call(
        functools.partial(gram_kernel, n_mem, n_chan, PARTS),
        out_shape=(jax.ShapeDtypeStruct((total, columns), F32),
                   jax.ShapeDtypeStruct((n_mem, members, states), BF16)),
        in_specs=[pl.BlockSpec(memory_space=pltpu.SMEM), anywhere, anywhere, vmem, anywhere],
        out_specs=(vmem, vmem),
        scratch_shapes=[
            pltpu.VMEM((n_mem, members, width), BF16),
            pltpu.VMEM((n_mem, members, states), BF16),
            pltpu.VMEM(innovation.shape, F32),
            pltpu.VMEM((n_chan, total, columns), F32),
            dma((3,)), dma((PARTS, n_mem)), dma((PARTS, n_mem)), dma((n_mem,)), dma((n_mem,)),
            dma((n_chan,)), dma((n_chan,)),
        ],
        compiler_params=pltpu.CompilerParams(
            collective_id=0, has_side_effects=True, vmem_limit_bytes=VMEM_LIMIT),
    )(valid_count, state_anom, radiance_anom, inv_noise, innovation)
    information, gradient, increment = pl.pallas_call(
        functools.partial(solve_kernel, total),
        out_shape=(jax.ShapeDtypeStruct((states, 1, states), F32),
                   jax.ShapeDtypeStruct((1, states), F32),
                   jax.ShapeDtypeStruct((1, states), F32)),
        in_specs=[vmem, vmem],
        out_specs=(vmem, vmem, vmem),
        compiler_params=pltpu.CompilerParams(vmem_limit_bytes=VMEM_LIMIT),
    )(gram, own_states)
    return information.transpose(1, 0, 2), gradient, increment


def solution(mesh):
    in_specs = (P(None, "mem", None), P(None, "mem", "chan"), P("chan"), P(None, "chan"), P())
    out_specs = (P("mem", None, None), P("mem", None), P("mem", None))
    return jax.shard_map(shards, mesh=mesh, in_specs=in_specs, out_specs=out_specs, check_vma=False)
```

```python
import functools
import jax
import jax.numpy as jnp
from jax import lax
from jax.experimental import pallas as pl
from jax.experimental.pallas import tpu as pltpu
from jax.sharding import PartitionSpec as P

F32, BF16 = jnp.float32, jnp.bfloat16
LANES, SUB = 128, 8
PARTS = 4
TINY = 2e-38
VMEM_LIMIT = 60 * 1024 * 1024


def up(x, to):
    return -(-x // to) * to


def split3(x):
    a = x.astype(BF16)
    rest = x - a.astype(F32)
    b = rest.astype(BF16)
    c = (rest - b.astype(F32)).astype(BF16)
    return a, b, c


def pieces(width, count):
    tiles = width // LANES
    marks = [(tiles - tiles * i // count) * LANES for i in range(count, 0, -1)] + [width]
    return list(zip(marks[:-1], marks[1:]))


def orthogonalise(anom, vectors_ref, lower_ref):
    total, states = anom.shape
    lanes = vectors_ref.shape[1]
    anom = jnp.concatenate([anom, jnp.zeros((total, lanes - states), F32)], 1)
    cid = lax.broadcasted_iota(jnp.int32, lower_ref.shape, 1)
    rid = lax.broadcasted_iota(jnp.int32, lower_ref.shape, 0)
    lower = jnp.zeros(lower_ref.shape, F32)
    for k in range(total):
        top = k // SUB * SUB
        live = anom[top:]
        vector = anom[k:k + 1]
        dots = jnp.sum(live * vector, axis=1, keepdims=True)
        norm = dots[k - top:k - top + 1]
        inverse = jnp.where(norm > TINY, 1.0 / norm, 0.0)
        after = lax.broadcasted_iota(jnp.int32, (total - top, 1), 0) > k - top
        live = live - jnp.where(after, dots * inverse, 0.0) * vector
        pad = [] if top == 0 else [jnp.zeros((top, 1), F32)]
        lower = jnp.where((cid == k) & (rid >= k), jnp.concatenate(pad + [dots], 0), lower)
        anom = live if top == 0 else jnp.concatenate([anom[:top], live], 0)
    diagonal = jnp.where(cid == rid, lower, 0.0)
    across = jnp.sum(diagonal, axis=0, keepdims=True)
    down = jnp.sum(diagonal, axis=1, keepdims=True)
    lower_ref[...] = lower * jnp.where(across > TINY, lax.rsqrt(across), 0.0)
    vectors_ref[...] = anom * jnp.where(down > TINY, lax.rsqrt(down), 0.0)


def gram_kernel(n_mem, n_chan, parts_of_slab, count_ref, state_ref, rad_ref, noise_ref, innov_ref,
                gram_ref, states_ref, *rest):
    basis_refs = rest[:-11]
    (held, held_states, innov, parts,
     local_sem, send_sem, recv_sem, ssend_sem, srecv_sem, psend_sem, precv_sem) = rest[-11:]
    me, slab = lax.axis_index("mem"), lax.axis_index("chan")
    members = rad_ref.shape[1]
    width = rad_ref.shape[2]
    total = n_mem * members
    columns = parts.shape[2]

    barrier = pltpu.get_barrier_semaphore()
    for k in range(1, n_mem):
        pl.semaphore_signal(barrier, inc=1, device_id={"mem": lax.rem(me + k, n_mem)})
    for k in range(1, n_chan):
        pl.semaphore_signal(barrier, inc=1, device_id={"chan": lax.rem(slab + k, n_chan)})
    own = [
        pltpu.make_async_copy(rad_ref.at[me], held.at[0], local_sem.at[0]),
        pltpu.make_async_copy(state_ref.at[me], held_states.at[0], local_sem.at[1]),
        pltpu.make_async_copy(innov_ref, innov, local_sem.at[2]),
    ]
    for copy in own:
        copy.start()
    for copy in own:
        copy.wait()
    slots = slab * width + lax.broadcasted_iota(jnp.int32, (1, width), 1)
    weight = jnp.where(slots < count_ref[me], noise_ref[...].reshape(1, width), 0.0)
    pull = weight * innov[pl.ds(me, 1), :]
    pull = [part.astype(F32) for part in split3(pull)]
    pl.semaphore_wait(barrier, n_mem - 1 + n_chan - 1)

    small = []
    for k in range(1, n_mem):
        peer = lax.rem(me + k, n_mem)
        small.append(pltpu.make_async_remote_copy(
            src_ref=state_ref.at[peer], dst_ref=held_states.at[k],
            send_sem=ssend_sem.at[k], recv_sem=srecv_sem.at[k], device_id={"mem": peer}))
        small[-1].start()
    cuts = pieces(width, parts_of_slab)
    sends, late = [], []
    for c, (lo, hi) in enumerate(cuts):
        for k in range(n_mem - 1, 0, -1):
            peer = lax.rem(me + k, n_mem)
            late.append(pltpu.make_async_remote_copy(
                src_ref=rad_ref.at[peer, :, lo:hi], dst_ref=held.at[k, :, lo:hi],
                send_sem=send_sem.at[c, k], recv_sem=recv_sem.at[c, k], device_id={"mem": peer}))
            late[-1].start()
        sends.append(late)
        late = []
    for copy in small:
        copy.wait_recv()
    states_ref[...] = held_states[...]
    if basis_refs:
        orthogonalise(held_states[...].astype(F32).reshape(total, held_states.shape[2]), *basis_refs)
    extra = columns - total
    row = lax.broadcasted_iota(jnp.int32, (extra, 1), 0)
    acc = jnp.zeros((total, columns), F32)
    step = 2 * LANES
    for (start, stop), copies in zip(cuts, sends):
        for copy in copies:
            copy.wait_recv()
        for lo in range(start, stop, step):
            hi = min(lo + step, stop)
            block = held[:, :, lo:hi].astype(F32).reshape(total, hi - lo)
            scaled = block * weight[:, lo:hi]
            first = scaled.astype(BF16)
            second = (scaled - first.astype(F32)).astype(BF16)
            p0, p1, p2 = (part[:, lo:hi] for part in pull)
            tail0 = jnp.where(row == 0, p0, jnp.where(row == 1, p2, 0.0)).astype(BF16)
            tail1 = jnp.where(row == 0, p1, 0.0).astype(BF16)
            block = block.astype(BF16)
            dims = (((1,), (1,)), ((), ()))
            acc += (
                lax.dot_general(block, jnp.concatenate([first, tail0], 0), dims, preferred_element_type=F32)
                + lax.dot_general(block, jnp.concatenate([second, tail1], 0), dims, preferred_element_type=F32)
            )
    parts[slab] = acc

    shares = []
    for k in range(1, n_chan):
        peer = lax.rem(slab + k, n_chan)
        shares.append(pltpu.make_async_remote_copy(
            src_ref=parts.at[slab], dst_ref=parts.at[slab],
            send_sem=psend_sem.at[k], recv_sem=precv_sem.at[k], device_id={"chan": peer}))
        shares[-1].start()
    for copy in small + sum(sends, []):
        copy.wait_send()
    for copy in shares:
        copy.wait()
    whole = parts[0]
    for k in range(1, n_chan):
        whole = whole + parts[k]
    gram_ref[...] = whole


def eliminate(system, order):
    rows, lanes = system.shape
    rid = lax.broadcasted_iota(jnp.int32, (SUB, LANES), 0)

    def wide(piece, tiles):
        return piece if tiles == 1 else jnp.concatenate([piece] * tiles, 1)

    for p in range(0, order, SUB):
        steps = min(SUB, order - p)
        base = p // LANES * LANES
        live = system[:, base:]
        tiles = (lanes - base) // LANES
        cols = []
        for j in range(steps):
            at = p - base + j
            full = jnp.broadcast_to(live[:, at:at + 1], (rows, LANES))
            cols.append([full[:p], full[p:p + SUB], full[p + SUB:]])
        block = live[p:p + SUB]
        above, below = live[:p], live[p + SUB:]
        for j in range(steps):
            inverse = 1.0 / cols[j][1][j:j + 1, :]
            pivot_row = block[j:j + 1, :] * wide(inverse, tiles)
            for later in range(j + 1, steps):
                c = cols[later]
                scale = c[1][j:j + 1, :] * inverse
                cols[later] = [
                    c[0] - cols[j][0] * scale if p else c[0],
                    jnp.where(rid == j, jnp.broadcast_to(scale, (SUB, LANES)), c[1] - cols[j][1] * scale),
                    c[2] - cols[j][2] * scale if p + SUB < rows else c[2],
                ]
            block = jnp.where(wide(rid, tiles) == j, jnp.broadcast_to(pivot_row, block.shape),
                              block - wide(cols[j][1], tiles) * pivot_row)
            if p:
                above = above - wide(cols[j][0], tiles) * pivot_row
            if p + SUB < rows:
                below = below - wide(cols[j][2], tiles) * pivot_row
        pieces = ([above] if p else []) + [block] + ([below] if p + SUB < rows else [])
        live = jnp.concatenate(pieces, 0) if len(pieces) > 1 else pieces[0]
        system = live if base == 0 else jnp.concatenate([system[:, :base], live], 1)
    return system[:, order:order + 1]


def solve_kernel(total, gram_ref, states_ref, *rest):
    basis_refs, (info_ref, grad_ref, inc_ref) = rest[:-3], rest[-3:]
    states = states_ref.shape[2]
    columns = gram_ref.shape[1]
    scale = 1.0 / (total - 1)
    rows, lanes = up(states, SUB), up(states + 1, LANES)
    anom = states_ref[...].astype(F32).reshape(total, states)
    anom = jnp.concatenate([anom, jnp.zeros((total, lanes - states), F32)], 1)
    gram = gram_ref[...]
    force = (gram[:, total:total + 1] + gram[:, total + 1:total + 2]) * scale
    grad_ref[...] = jnp.sum(force * anom, axis=0, keepdims=True)[:, :states]
    if basis_refs:
        vectors_ref, lower_ref = basis_refs
        lower = lower_ref[...]
        order = lower.T[:total]
        mixed = jnp.dot(order, gram, precision=lax.Precision.HIGHEST, preferred_element_type=F32)
        right = (mixed[:, total:total + 1] + mixed[:, total + 1:total + 2]) * scale
        full = jnp.concatenate([lower, jnp.zeros((columns - total, lower.shape[1]), F32)], 0)
        system = jnp.dot(mixed, full, precision=lax.Precision.HIGHEST, preferred_element_type=F32) * (scale * scale)
        rid = lax.broadcasted_iota(jnp.int32, system.shape, 0)
        cid = lax.broadcasted_iota(jnp.int32, system.shape, 1)
        system = system + jnp.where(rid == cid, 1.0, 0.0)
        system = jnp.where(cid == total, jnp.broadcast_to(right, system.shape), system)
        step = eliminate(system, total)
        inc_ref[...] = jnp.sum(step * vectors_ref[...], axis=0, keepdims=True)[:, :states]
    turned = anom.T[:rows].astype(BF16)
    anom = jnp.concatenate([anom, jnp.zeros((columns - total, lanes), F32)], 0).astype(BF16)
    half = functools.reduce(
        lambda a, b: b + a,
        [jnp.dot(turned, g, preferred_element_type=F32) for g in split3(gram)][::-1])
    grad = (half[:, total:total + 1] + half[:, total + 1:total + 2]) * scale
    info = functools.reduce(
        lambda a, b: b + a,
        [jnp.dot(h, anom, preferred_element_type=F32) for h in split3(half)][::-1])
    info = info * (scale * scale)
    info_ref[:, 0, :] = info[:states, :states]
    if basis_refs:
        return
    rid = lax.broadcasted_iota(jnp.int32, (rows, lanes), 0)
    cid = lax.broadcasted_iota(jnp.int32, (rows, lanes), 1)
    system = info + jnp.where(rid == cid, 1.0, 0.0)
    system = jnp.where(cid == states, jnp.broadcast_to(grad, (rows, lanes)), system)
    step = eliminate(system, states)
    lid = lax.broadcasted_iota(jnp.int32, (rows, LANES), 1)
    pair = jnp.where(lid == 1, step, 0.0)
    pair = jnp.concatenate([pair, jnp.zeros((lanes - rows, LANES), F32)], 0).T
    inc_ref[...] = pair[1:2, :states]


def shards(state_anom, radiance_anom, inv_noise, innovation, valid_count):
    n_mem, n_chan = lax.axis_size("mem"), lax.axis_size("chan")
    members, states = state_anom.shape[1:]
    width = radiance_anom.shape[2]
    total = members * n_mem
    columns = up(total + 16, LANES)
    vmem, anywhere = pl.BlockSpec(memory_space=pltpu.VMEM), pl.BlockSpec(memory_space=pl.ANY)
    dma = pltpu.SemaphoreType.DMA
    basis = () if total > states else (jax.ShapeDtypeStruct((total, up(states + 1, LANES)), F32),
                                       jax.ShapeDtypeStruct((total, up(total + 1, LANES)), F32))
    gram, own_states, *bases = pl.pallas_call(
        functools.partial(gram_kernel, n_mem, n_chan, PARTS),
        out_shape=(jax.ShapeDtypeStruct((total, columns), F32),
                   jax.ShapeDtypeStruct((n_mem, members, states), BF16)) + basis,
        in_specs=[pl.BlockSpec(memory_space=pltpu.SMEM), anywhere, anywhere, vmem, anywhere],
        out_specs=(vmem,) * (2 + len(basis)),
        scratch_shapes=[
            pltpu.VMEM((n_mem, members, width), BF16),
            pltpu.VMEM((n_mem, members, states), BF16),
            pltpu.VMEM(innovation.shape, F32),
            pltpu.VMEM((n_chan, total, columns), F32),
            dma((3,)), dma((PARTS, n_mem)), dma((PARTS, n_mem)), dma((n_mem,)), dma((n_mem,)),
            dma((n_chan,)), dma((n_chan,)),
        ],
        compiler_params=pltpu.CompilerParams(
            collective_id=0, has_side_effects=True, vmem_limit_bytes=VMEM_LIMIT),
    )(valid_count, state_anom, radiance_anom, inv_noise, innovation)
    information, gradient, increment = pl.pallas_call(
        functools.partial(solve_kernel, total),
        out_shape=(jax.ShapeDtypeStruct((states, 1, states), F32),
                   jax.ShapeDtypeStruct((1, states), F32),
                   jax.ShapeDtypeStruct((1, states), F32)),
        in_specs=[vmem] * (2 + len(basis)),
        out_specs=(vmem, vmem, vmem),
        compiler_params=pltpu.CompilerParams(vmem_limit_bytes=VMEM_LIMIT),
    )(gram, own_states, *bases)
    return information.transpose(1, 0, 2), gradient, increment


def solution(mesh):
    in_specs = (P(None, "mem", None), P(None, "mem", "chan"), P("chan"), P(None, "chan"), P())
    out_specs = (P("mem", None, None), P("mem", None), P("mem", None))
    return jax.shard_map(shards, mesh=mesh, in_specs=in_specs, out_specs=out_specs, check_vma=False)
```

```python
import functools
import jax
import jax.numpy as jnp
from jax import lax
from jax.experimental import pallas as pl
from jax.experimental.pallas import tpu as pltpu
from jax.sharding import PartitionSpec as P

F32, BF16 = jnp.float32, jnp.bfloat16
LANES, SUB = 128, 8
PARTS = 4
TINY = 2e-38
VMEM_LIMIT = 60 * 1024 * 1024


def up(x, to):
    return -(-x // to) * to


def split3(x):
    a = x.astype(BF16)
    rest = x - a.astype(F32)
    b = rest.astype(BF16)
    c = (rest - b.astype(F32)).astype(BF16)
    return a, b, c


def pieces(width, count):
    tiles = width // LANES
    marks = [(tiles - tiles * i // count) * LANES for i in range(count, 0, -1)] + [width]
    return list(zip(marks[:-1], marks[1:]))


def orthogonalise(state, first, last):
    anom, lower = state
    total = anom.shape[0]
    cid = lax.broadcasted_iota(jnp.int32, lower.shape, 1)
    rid = lax.broadcasted_iota(jnp.int32, lower.shape, 0)
    for k in range(first, last):
        top = k // SUB * SUB
        live = anom[top:]
        vector = anom[k:k + 1]
        dots = jnp.sum(live * vector, axis=1, keepdims=True)
        norm = dots[k - top:k - top + 1]
        inverse = jnp.where(norm > TINY, 1.0 / norm, 0.0)
        after = lax.broadcasted_iota(jnp.int32, (total - top, 1), 0) > k - top
        live = live - jnp.where(after, dots * inverse, 0.0) * vector
        pad = [] if top == 0 else [jnp.zeros((top, 1), F32)]
        lower = jnp.where((cid == k) & (rid >= k), jnp.concatenate(pad + [dots], 0), lower)
        anom = live if top == 0 else jnp.concatenate([anom[:top], live], 0)
    return anom, lower


def normalise(state, vectors_ref, lower_ref):
    anom, lower = state
    cid = lax.broadcasted_iota(jnp.int32, lower.shape, 1)
    rid = lax.broadcasted_iota(jnp.int32, lower.shape, 0)
    diagonal = jnp.where(cid == rid, lower, 0.0)
    across = jnp.sum(diagonal, axis=0, keepdims=True)
    down = jnp.sum(diagonal, axis=1, keepdims=True)
    lower_ref[...] = lower * jnp.where(across > TINY, lax.rsqrt(across), 0.0)
    vectors_ref[...] = anom * jnp.where(down > TINY, lax.rsqrt(down), 0.0)


def gram_kernel(n_mem, n_chan, parts_of_slab, count_ref, state_ref, rad_ref, noise_ref, innov_ref,
                gram_ref, states_ref, *rest):
    basis_refs = rest[:-11]
    (held, held_states, innov, parts,
     local_sem, send_sem, recv_sem, ssend_sem, srecv_sem, psend_sem, precv_sem) = rest[-11:]
    me, slab = lax.axis_index("mem"), lax.axis_index("chan")
    members = rad_ref.shape[1]
    width = rad_ref.shape[2]
    total = n_mem * members
    columns = parts.shape[2]

    barrier = pltpu.get_barrier_semaphore()
    for k in range(1, n_mem):
        pl.semaphore_signal(barrier, inc=1, device_id={"mem": lax.rem(me + k, n_mem)})
    for k in range(1, n_chan):
        pl.semaphore_signal(barrier, inc=1, device_id={"chan": lax.rem(slab + k, n_chan)})
    own = [
        pltpu.make_async_copy(rad_ref.at[me], held.at[0], local_sem.at[0]),
        pltpu.make_async_copy(state_ref.at[me], held_states.at[0], local_sem.at[1]),
        pltpu.make_async_copy(innov_ref, innov, local_sem.at[2]),
    ]
    for copy in own:
        copy.start()
    for copy in own:
        copy.wait()
    slots = slab * width + lax.broadcasted_iota(jnp.int32, (1, width), 1)
    weight = jnp.where(slots < count_ref[me], noise_ref[...].reshape(1, width), 0.0)
    pull = weight * innov[pl.ds(me, 1), :]
    pull = [part.astype(F32) for part in split3(pull)]
    pl.semaphore_wait(barrier, n_mem - 1 + n_chan - 1)

    small = []
    for k in range(1, n_mem):
        peer = lax.rem(me + k, n_mem)
        small.append(pltpu.make_async_remote_copy(
            src_ref=state_ref.at[peer], dst_ref=held_states.at[k],
            send_sem=ssend_sem.at[k], recv_sem=srecv_sem.at[k], device_id={"mem": peer}))
        small[-1].start()
    cuts = pieces(width, parts_of_slab)
    sends, late = [], []
    for c, (lo, hi) in enumerate(cuts):
        for k in range(n_mem - 1, 0, -1):
            peer = lax.rem(me + k, n_mem)
            late.append(pltpu.make_async_remote_copy(
                src_ref=rad_ref.at[peer, :, lo:hi], dst_ref=held.at[k, :, lo:hi],
                send_sem=send_sem.at[c, k], recv_sem=recv_sem.at[c, k], device_id={"mem": peer}))
            late[-1].start()
        sends.append(late)
        late = []
    for copy in small:
        copy.wait_recv()
    states_ref[...] = held_states[...]
    if basis_refs:
        anom = held_states[...].astype(F32).reshape(total, held_states.shape[2])
        spare = jnp.zeros((total, basis_refs[0].shape[1] - anom.shape[1]), F32)
        basis = jnp.concatenate([anom, spare], 1), jnp.zeros(basis_refs[1].shape, F32)
        early = total * 7 // 16
        basis = orthogonalise(basis, 0, early)
    extra = columns - total
    row = lax.broadcasted_iota(jnp.int32, (extra, 1), 0)
    acc = jnp.zeros((total, columns), F32)
    step = 2 * LANES
    for (start, stop), copies in zip(cuts, sends):
        for copy in copies:
            copy.wait_recv()
        for lo in range(start, stop, step):
            hi = min(lo + step, stop)
            block = held[:, :, lo:hi].astype(F32).reshape(total, hi - lo)
            scaled = block * weight[:, lo:hi]
            first = scaled.astype(BF16)
            second = (scaled - first.astype(F32)).astype(BF16)
            p0, p1, p2 = (part[:, lo:hi] for part in pull)
            tail0 = jnp.where(row == 0, p0, jnp.where(row == 1, p2, 0.0)).astype(BF16)
            tail1 = jnp.where(row == 0, p1, 0.0).astype(BF16)
            block = block.astype(BF16)
            dims = (((1,), (1,)), ((), ()))
            acc += (
                lax.dot_general(block, jnp.concatenate([first, tail0], 0), dims, preferred_element_type=F32)
                + lax.dot_general(block, jnp.concatenate([second, tail1], 0), dims, preferred_element_type=F32)
            )
    parts[slab] = acc

    shares = []
    for k in range(1, n_chan):
        peer = lax.rem(slab + k, n_chan)
        shares.append(pltpu.make_async_remote_copy(
            src_ref=parts.at[slab], dst_ref=parts.at[slab],
            send_sem=psend_sem.at[k], recv_sem=precv_sem.at[k], device_id={"chan": peer}))
        shares[-1].start()
    if basis_refs:
        normalise(orthogonalise(basis, early, total), *basis_refs)
    for copy in small + sum(sends, []):
        copy.wait_send()
    for copy in shares:
        copy.wait()
    whole = parts[0]
    for k in range(1, n_chan):
        whole = whole + parts[k]
    gram_ref[...] = whole


def eliminate(system, order):
    rows, lanes = system.shape
    rid = lax.broadcasted_iota(jnp.int32, (SUB, LANES), 0)

    def wide(piece, tiles):
        return piece if tiles == 1 else jnp.concatenate([piece] * tiles, 1)

    for p in range(0, order, SUB):
        steps = min(SUB, order - p)
        base = p // LANES * LANES
        live = system[:, base:]
        tiles = (lanes - base) // LANES
        cols = []
        for j in range(steps):
            at = p - base + j
            full = jnp.broadcast_to(live[:, at:at + 1], (rows, LANES))
            cols.append([full[:p], full[p:p + SUB], full[p + SUB:]])
        block = live[p:p + SUB]
        above, below = live[:p], live[p + SUB:]
        for j in range(steps):
            inverse = 1.0 / cols[j][1][j:j + 1, :]
            pivot_row = block[j:j + 1, :] * wide(inverse, tiles)
            for later in range(j + 1, steps):
                c = cols[later]
                scale = c[1][j:j + 1, :] * inverse
                cols[later] = [
                    c[0] - cols[j][0] * scale if p else c[0],
                    jnp.where(rid == j, jnp.broadcast_to(scale, (SUB, LANES)), c[1] - cols[j][1] * scale),
                    c[2] - cols[j][2] * scale if p + SUB < rows else c[2],
                ]
            block = jnp.where(wide(rid, tiles) == j, jnp.broadcast_to(pivot_row, block.shape),
                              block - wide(cols[j][1], tiles) * pivot_row)
            if p:
                above = above - wide(cols[j][0], tiles) * pivot_row
            if p + SUB < rows:
                below = below - wide(cols[j][2], tiles) * pivot_row
        pieces = ([above] if p else []) + [block] + ([below] if p + SUB < rows else [])
        live = jnp.concatenate(pieces, 0) if len(pieces) > 1 else pieces[0]
        system = live if base == 0 else jnp.concatenate([system[:, :base], live], 1)
    return system[:, order:order + 1]


def solve_kernel(total, gram_ref, states_ref, *rest):
    basis_refs, (info_ref, grad_ref, inc_ref) = rest[:-3], rest[-3:]
    states = states_ref.shape[2]
    columns = gram_ref.shape[1]
    scale = 1.0 / (total - 1)
    rows, lanes = up(states, SUB), up(states + 1, LANES)
    anom = states_ref[...].astype(F32).reshape(total, states)
    anom = jnp.concatenate([anom, jnp.zeros((total, lanes - states), F32)], 1)
    gram = gram_ref[...]
    force = (gram[:, total:total + 1] + gram[:, total + 1:total + 2]) * scale
    grad_ref[...] = jnp.sum(force * anom, axis=0, keepdims=True)[:, :states]
    if basis_refs:
        vectors_ref, lower_ref = basis_refs
        lower = lower_ref[...]
        order = lower.T[:total]
        mixed = jnp.dot(order, gram, precision=lax.Precision.HIGHEST, preferred_element_type=F32)
        right = (mixed[:, total:total + 1] + mixed[:, total + 1:total + 2]) * scale
        full = jnp.concatenate([lower, jnp.zeros((columns - total, lower.shape[1]), F32)], 0)
        system = jnp.dot(mixed, full, precision=lax.Precision.HIGHEST, preferred_element_type=F32) * (scale * scale)
        rid = lax.broadcasted_iota(jnp.int32, system.shape, 0)
        cid = lax.broadcasted_iota(jnp.int32, system.shape, 1)
        system = system + jnp.where(rid == cid, 1.0, 0.0)
        system = jnp.where(cid == total, jnp.broadcast_to(right, system.shape), system)
        step = eliminate(system, total)
        inc_ref[...] = jnp.sum(step * vectors_ref[...], axis=0, keepdims=True)[:, :states]
    turned = anom.T[:rows].astype(BF16)
    anom = jnp.concatenate([anom, jnp.zeros((columns - total, lanes), F32)], 0).astype(BF16)
    half = functools.reduce(
        lambda a, b: b + a,
        [jnp.dot(turned, g, preferred_element_type=F32) for g in split3(gram)][::-1])
    grad = (half[:, total:total + 1] + half[:, total + 1:total + 2]) * scale
    info = functools.reduce(
        lambda a, b: b + a,
        [jnp.dot(h, anom, preferred_element_type=F32) for h in split3(half)][::-1])
    info = info * (scale * scale)
    info_ref[:, 0, :] = info[:states, :states]
    if basis_refs:
        return
    rid = lax.broadcasted_iota(jnp.int32, (rows, lanes), 0)
    cid = lax.broadcasted_iota(jnp.int32, (rows, lanes), 1)
    system = info + jnp.where(rid == cid, 1.0, 0.0)
    system = jnp.where(cid == states, jnp.broadcast_to(grad, (rows, lanes)), system)
    step = eliminate(system, states)
    lid = lax.broadcasted_iota(jnp.int32, (rows, LANES), 1)
    pair = jnp.where(lid == 1, step, 0.0)
    pair = jnp.concatenate([pair, jnp.zeros((lanes - rows, LANES), F32)], 0).T
    inc_ref[...] = pair[1:2, :states]


def shards(state_anom, radiance_anom, inv_noise, innovation, valid_count):
    n_mem, n_chan = lax.axis_size("mem"), lax.axis_size("chan")
    members, states = state_anom.shape[1:]
    width = radiance_anom.shape[2]
    total = members * n_mem
    columns = up(total + 16, LANES)
    vmem, anywhere = pl.BlockSpec(memory_space=pltpu.VMEM), pl.BlockSpec(memory_space=pl.ANY)
    dma = pltpu.SemaphoreType.DMA
    basis = () if total > states else (jax.ShapeDtypeStruct((total, up(states + 1, LANES)), F32),
                                       jax.ShapeDtypeStruct((total, up(total + 1, LANES)), F32))
    gram, own_states, *bases = pl.pallas_call(
        functools.partial(gram_kernel, n_mem, n_chan, PARTS),
        out_shape=(jax.ShapeDtypeStruct((total, columns), F32),
                   jax.ShapeDtypeStruct((n_mem, members, states), BF16)) + basis,
        in_specs=[pl.BlockSpec(memory_space=pltpu.SMEM), anywhere, anywhere, vmem, anywhere],
        out_specs=(vmem,) * (2 + len(basis)),
        scratch_shapes=[
            pltpu.VMEM((n_mem, members, width), BF16),
            pltpu.VMEM((n_mem, members, states), BF16),
            pltpu.VMEM(innovation.shape, F32),
            pltpu.VMEM((n_chan, total, columns), F32),
            dma((3,)), dma((PARTS, n_mem)), dma((PARTS, n_mem)), dma((n_mem,)), dma((n_mem,)),
            dma((n_chan,)), dma((n_chan,)),
        ],
        compiler_params=pltpu.CompilerParams(
            collective_id=0, has_side_effects=True, vmem_limit_bytes=VMEM_LIMIT),
    )(valid_count, state_anom, radiance_anom, inv_noise, innovation)
    information, gradient, increment = pl.pallas_call(
        functools.partial(solve_kernel, total),
        out_shape=(jax.ShapeDtypeStruct((states, 1, states), F32),
                   jax.ShapeDtypeStruct((1, states), F32),
                   jax.ShapeDtypeStruct((1, states), F32)),
        in_specs=[vmem] * (2 + len(basis)),
        out_specs=(vmem, vmem, vmem),
        compiler_params=pltpu.CompilerParams(vmem_limit_bytes=VMEM_LIMIT),
    )(gram, own_states, *bases)
    return information.transpose(1, 0, 2), gradient, increment


def solution(mesh):
    in_specs = (P(None, "mem", None), P(None, "mem", "chan"), P("chan"), P(None, "chan"), P())
    out_specs = (P("mem", None, None), P("mem", None), P("mem", None))
    return jax.shard_map(shards, mesh=mesh, in_specs=in_specs, out_specs=out_specs, check_vma=False)
```
